32 devices in a mesh: task: 4 (over y, x), tp: 8 (over z, core).
Axes of the slice: x: 2, y: 2, z: 4, core: 2. Of those that a mesh axis runs over, the one named last changes fastest.
Arguments:
- observations: bfloat16 [128, 16, 4096], P('task', None, 'tp'), may hold values from -6 to 6
- gain: float32 [4096], P('tp'), may hold values from 0.5 to 1.5
- w_in: bfloat16 [4096, 4096], P(None, 'tp'), may hold values from -0.09375 to 0.09375
- w_mix: bfloat16 [4096, 4096], P('tp'), may hold values from -0.09375 to 0.09375
- w_out: bfloat16 [4096, 4096], P(None, 'tp'), may hold values from -0.09375 to 0.09375
- w_head: bfloat16 [4096, 75], P('tp'), may hold values from -0.09375 to 0.09375
- head_bias: float32 [75], replicated, may hold values from -4 to 4
- pop_mean: float32 [57], replicated, may hold values from -8 to 8
- pop_scale: float32 [57], replicated, may hold values from 0.5 to 4
- task_indices: int32 [128], P('task'), may hold values from 0 to 56
- actions: int32 [128, 15], P('task'), may hold values from 0 to 17
- rewards: float32 [128, 15], P('task'), may hold values from -18 to 27
- episode_ends: int32 [128, 15], P('task'), may hold values 0 or 1
- behaviour_log_prob: float32 [128, 15], P('task'), may hold values from -4.5 to -1.5
Outputs:
- grad_w_in: float32 [4096, 4096], P(None, 'tp')
- grad_w_mix: float32 [4096, 4096], P('tp')
- grad_w_out: float32 [4096, 4096], P(None, 'tp')
- grad_gain: float32 [4096], P('tp')
- grad_head: float32 [4096, 75], P('tp')
- grad_head_bias: float32 [75], replicated
- new_head: bfloat16 [4096, 75], P('tp')
- new_bias: float32 [75], replicated
- updated_return_mean: float32 [57], replicated
- updated_return_scale: float32 [57], replicated
The draws below stay inside these ranges and needn't reach their ends.
All inputs are finite; a program needn't handle non-finite values. No bound on the sum of `episode_ends` on one device may be relied on, other than what follows from the above.
Results may differ from the reference program's by a relative error of at most 0.03.
Values may be sent and summed in bfloat16 or wider, within the bound.
No kernel may reach another device: no remote copies, remote signals or barrier semaphores. Data moves between devices by JAX's collectives and lax.ppermute only.
A program may use at most 128 MiB of HBM per device.

```python
import math
import jax
import jax.numpy as jnp
from jax import lax

D = 4096
ACTIONS = 18
TASKS = 57
HEADS = 75
B_DEV = 32
FRAMES = 16
UNROLL = 15
ENVS = 128
N_TP = 8


def draw_rewards(key, part):
    group_index = (jnp.arange(ENVS, dtype=jnp.int32) // B_DEV).astype(jnp.float32)
    last_group = max(ENVS // B_DEV - 1, 1)
    rising = 1.0 + 2.0 * group_index / last_group
    sample = jnp.clip(jax.random.normal(key, (ENVS, UNROLL), jnp.float32), -4.0, 4.0)
    return sample * rising[:, None]


def set_ends(values, key, least, top_value):
    longest = values.shape.index(max(values.shape))
    spots = []
    for shift in (0, 1):
        where = [jax.random.randint(jax.random.fold_in(key, axis), (), 0, length) for axis, length in enumerate(values.shape)]
        where[longest] = (where[longest] + shift) % values.shape[longest]
        spots.append(tuple(where))
    return values.at[spots[0]].set(least).at[spots[1]].set(top_value)


def shard_levels(own_key, shape, shards, low, top_value):
    def one(axis_at, shards_of):
        heights = jax.random.uniform(jax.random.fold_in(jax.random.fold_in(own_key, 6), axis_at), (shards_of,), jnp.float32, low / len(shards), top_value / len(shards))
        return jnp.repeat(jnp.exp(heights), shape[axis_at] // shards_of).reshape((-1,) + (1,) * (len(shape) - axis_at - 1))

    loudness = one(*shards[0])
    for cut in shards[1:]:
        loudness = loudness * one(*cut)
    return loudness


def bell_draw(rng, extent, width, most, split=(), held_as=jnp.bfloat16):
    entries = width * jax.random.normal(rng, extent, jnp.float32)
    if split:
        entries = entries * shard_levels(rng, extent, split, -0.22, 0.18)
    return jnp.clip(entries, -most, most).astype(held_as)


def setup_inputs(seed: int = 0) -> dict:
    keys = jax.random.split(jax.random.key(seed), 15)
    observations = bell_draw(keys[0], (ENVS, FRAMES, D), 1.0, 6.0, ((0, 4), (2, 8)))
    gain = jnp.clip(1.0 + 0.1 * jax.random.normal(keys[1], (D,), jnp.float32), 0.5, 1.5)
    w_in = bell_draw(keys[2], (D, D), D ** -0.5, 0.09375, ((1, 8),))
    w_mix = bell_draw(keys[3], (D, D), D ** -0.5, 0.09375, ((0, 8),))
    w_out = bell_draw(keys[4], (D, D), D ** -0.5, 0.09375, ((1, 8),))
    w_head = bell_draw(keys[5], (D, HEADS), D ** -0.5, 0.09375, ((0, 8),))
    head_bias = bell_draw(keys[6], (HEADS,), 1.0, 4.0, (), jnp.float32)
    pop_mean = bell_draw(keys[7], (TASKS,), 2.0, 8.0, (), jnp.float32)
    pop_scale = jnp.clip(jnp.exp(jax.random.uniform(keys[8], (TASKS,), jnp.float32, math.log(0.5), math.log(4.0))), 0.5, 4.0)
    task_indices = set_ends(jax.random.randint(keys[9], (ENVS,), 0, TASKS), jax.random.fold_in(keys[9], 1), 0, TASKS - 1).astype(jnp.int32)
    actions = set_ends(jax.random.randint(keys[10], (ENVS, UNROLL), 0, ACTIONS), jax.random.fold_in(keys[10], 1), 0, ACTIONS - 1).astype(jnp.int32)
    rewards = draw_rewards(jax.random.fold_in(keys[14], 71), 0)
    episode_ends = set_ends((jax.random.randint(keys[12], (ENVS, UNROLL), 0, 16) < 1).astype(jnp.int32), jax.random.fold_in(keys[12], 1), 0, 1)
    behaviour_log_prob = jnp.clip(-4.5 + 3.0 * jax.random.uniform(keys[13], (ENVS, UNROLL), jnp.float32) ** shard_levels(keys[13], (ENVS, UNROLL), ((0, 4),), -0.2, 0.2), -4.5, -1.5)
    return dict(observations=observations, gain=gain, w_in=w_in, w_mix=w_mix, w_out=w_out, w_head=w_head, head_bias=head_bias, pop_mean=pop_mean, pop_scale=pop_scale, task_indices=task_indices, actions=actions, rewards=rewards, episode_ends=episode_ends, behaviour_log_prob=behaviour_log_prob)


DISCOUNT = 0.99
BASELINE_COST = 0.5
ENTROPY_COST = 0.01
POPART_PRIOR = 64.0
NORM_EPS = 1e-06

def silu_slope(before):
    sigmoid = jax.nn.sigmoid(before)
    return sigmoid * (1.0 + before * (1.0 - sigmoid))

def discounted_sums(values, factors):

    def advance(running, column):
        latest = column[0] + column[1] * running
        return (latest, latest)
    opening = jnp.zeros((values.shape[0],), jnp.float32)
    ending, stacked = lax.scan(advance, opening, (values.T, factors.T), reverse=True)
    return stacked.T

def task_onehot(task_indices):
    return (task_indices[:, None] == jnp.arange(TASKS, dtype=jnp.int32)[None, :]).astype(jnp.float32)

def popart_partials(task_indices, rewards, discount_factors):
    returns = discounted_sums(rewards, discount_factors)
    task_table = task_onehot(task_indices)
    counts = lax.optimization_barrier(jnp.sum(task_table, axis=0)) * rewards.shape[1]
    totals = jnp.dot(task_table.T, lax.optimization_barrier(jnp.sum(returns, axis=1)), precision=lax.Precision.HIGHEST)
    squares = jnp.dot(task_table.T, lax.optimization_barrier(jnp.sum(returns * returns, axis=1)), precision=lax.Precision.HIGHEST)
    return (counts, totals, squares)

def popart_update(counts, totals, squares, pop_mean, pop_scale):
    mixing = counts / (counts + POPART_PRIOR)
    safe_counts = jnp.maximum(counts, 1.0)
    batch_mean = totals / safe_counts
    batch_square = squares / safe_counts
    updated_return_mean = (1.0 - mixing) * pop_mean + mixing * batch_mean
    mean_gap = batch_mean - pop_mean
    variance = (1.0 - mixing) * pop_scale * pop_scale + mixing * (batch_square - batch_mean * batch_mean) + mixing * (1.0 - mixing) * mean_gap * mean_gap
    return (updated_return_mean, jnp.sqrt(variance))

def rescale_head(w_head, head_bias, pop_mean, pop_scale, updated_return_mean, updated_return_scale):
    scale_ratio = pop_scale / updated_return_scale
    column_scale = jnp.concatenate([jnp.ones((ACTIONS,), jnp.float32), scale_ratio])
    new_head = (w_head.astype(jnp.float32) * column_scale[None, :]).astype(jnp.bfloat16)
    value_bias = (pop_scale * head_bias[ACTIONS:] + pop_mean - updated_return_mean) / updated_return_scale
    new_bias = jnp.concatenate([head_bias[:ACTIONS], value_bias])
    return (new_head, new_bias)

def importance_trace_loss(head_value_estimates, task_indices, actions, rewards, discount_factors, behaviour_log_prob, updated_return_mean, updated_return_scale, loss_weighting):
    task_table = task_onehot(task_indices)
    env_mean = jnp.dot(task_table, updated_return_mean, precision=lax.Precision.HIGHEST)[:, None]
    env_scale = jnp.dot(task_table, updated_return_scale, precision=lax.Precision.HIGHEST)[:, None]
    logits = head_value_estimates[:, :-1, :ACTIONS]
    norm_values = lax.optimization_barrier(jnp.sum(head_value_estimates[:, :, ACTIONS:] * task_table[:, None, :], axis=2))
    values = lax.stop_gradient(norm_values * env_scale + env_mean)
    log_total = jnp.log(lax.optimization_barrier(jnp.sum(jnp.exp(logits), axis=2)))
    chosen = actions[:, :, None] == jnp.arange(ACTIONS, dtype=jnp.int32)[None, None, :]
    log_policy = lax.optimization_barrier(jnp.sum(jnp.where(chosen, logits, 0.0), axis=2)) - log_total
    clipped = jnp.minimum(jnp.exp(lax.stop_gradient(log_policy) - behaviour_log_prob), 1.0)
    deltas = clipped * (rewards + discount_factors * values[:, 1:] - values[:, :-1])
    targets = values[:, :-1] + discounted_sums(deltas, discount_factors * clipped)
    following = jnp.concatenate([targets[:, 1:], values[:, -1:]], axis=1)
    advantage = lax.stop_gradient(clipped * ((rewards + discount_factors * following - env_mean) / env_scale - norm_values[:, :-1]))
    normed_targets = lax.stop_gradient((targets - env_mean) / env_scale)
    policy = jnp.exp(logits - log_total[:, :, None])
    entropy = -lax.optimization_barrier(jnp.sum(policy * (logits - log_total[:, :, None]), axis=2))
    per_frame = -advantage * log_policy + 0.5 * BASELINE_COST * (normed_targets - norm_values[:, :-1]) ** 2 - ENTROPY_COST * entropy
    return loss_weighting * jnp.sum(per_frame)

def reference(observations, gain, w_in, w_mix, w_out, w_head, head_bias, pop_mean, pop_scale, task_indices, actions, rewards, episode_ends, behaviour_log_prob):
    env_count, frames, full_width = observations.shape
    block_width = full_width // N_TP
    row_count = env_count * frames
    tokens = observations.reshape(row_count, full_width)
    pre_in = jnp.dot(tokens, w_in, preferred_element_type=jnp.float32)
    hidden_in = jax.nn.silu(pre_in).astype(jnp.bfloat16)

    def mix_block(running, block_index):
        hidden_block = lax.dynamic_slice_in_dim(hidden_in, block_index * block_width, block_width, 1)
        weight_block = lax.dynamic_slice_in_dim(w_mix, block_index * block_width, block_width, 0)
        block_product = lax.optimization_barrier(jnp.dot(hidden_block, weight_block, preferred_element_type=jnp.float32).astype(jnp.bfloat16))
        return (running + block_product.astype(jnp.float32), None)
    mix_sum, unused = lax.scan(mix_block, jnp.zeros((row_count, full_width), jnp.float32), jnp.arange(N_TP, dtype=jnp.int32))
    residual = tokens.astype(jnp.float32) + mix_sum
    inverse = lax.rsqrt(lax.optimization_barrier(jnp.mean(residual * residual, axis=1, keepdims=True)) + NORM_EPS)
    normed = (residual * inverse * gain[None, :]).astype(jnp.bfloat16)
    pre_out = jnp.dot(normed, w_out, preferred_element_type=jnp.float32)
    hidden_out = jax.nn.silu(pre_out).astype(jnp.bfloat16)
    discount_factors = DISCOUNT * (1.0 - episode_ends.astype(jnp.float32))
    counts, totals, squares = popart_partials(task_indices, rewards, discount_factors)
    updated_return_mean, updated_return_scale = popart_update(counts, totals, squares, pop_mean, pop_scale)
    new_head, new_bias = rescale_head(w_head, head_bias, pop_mean, pop_scale, updated_return_mean, updated_return_scale)
    head_value_estimates = jnp.dot(hidden_out, new_head, preferred_element_type=jnp.float32) + new_bias[None, :]
    head_value_estimates = head_value_estimates.reshape(env_count, frames, -1)
    loss_weighting = float(ENVS) ** (-0.5)

    def whole_loss(network_outputs):
        return importance_trace_loss(network_outputs, task_indices, actions, rewards, discount_factors, behaviour_log_prob, updated_return_mean, updated_return_scale, loss_weighting)
    loss_value, pullback = jax.vjp(whole_loss, head_value_estimates)
    d_heads, = pullback(jnp.ones((), jnp.float32))
    d_rounded = d_heads.reshape(row_count, -1).astype(jnp.bfloat16)
    grad_head = jnp.dot(hidden_out.T, d_rounded, preferred_element_type=jnp.float32)
    grad_bias = lax.optimization_barrier(jnp.sum(d_rounded.astype(jnp.float32), axis=0))
    d_hidden_out = jnp.dot(d_rounded, new_head.T, preferred_element_type=jnp.float32)
    d_pre_out = (d_hidden_out * silu_slope(pre_out)).astype(jnp.bfloat16)
    grad_out = jnp.dot(normed.T, d_pre_out, preferred_element_type=jnp.float32)

    def back_block(running, block_index):
        grad_block = lax.dynamic_slice_in_dim(d_pre_out, block_index * block_width, block_width, 1)
        weight_block = lax.dynamic_slice_in_dim(w_out, block_index * block_width, block_width, 1)
        block_product = lax.optimization_barrier(jnp.dot(grad_block, weight_block.T, preferred_element_type=jnp.float32).astype(jnp.bfloat16))
        return (running + block_product.astype(jnp.float32), None)
    d_normed, unused = lax.scan(back_block, jnp.zeros((row_count, full_width), jnp.float32), jnp.arange(N_TP, dtype=jnp.int32))
    scaled = d_normed * gain[None, :]
    inner_sum = lax.optimization_barrier(jnp.sum(scaled * residual, axis=1, keepdims=True))
    d_residual = (inverse * scaled - residual * inverse ** 3 * inner_sum / full_width).astype(jnp.bfloat16)
    grad_gain = lax.optimization_barrier(jnp.sum(d_normed * residual * inverse, axis=0))
    grad_mix = jnp.dot(hidden_in.T, d_residual, preferred_element_type=jnp.float32)
    d_hidden_in = jnp.dot(d_residual, w_mix.T, preferred_element_type=jnp.float32)
    d_pre_in = (d_hidden_in * silu_slope(pre_in)).astype(jnp.bfloat16)
    grad_in = jnp.dot(tokens.T, d_pre_in, preferred_element_type=jnp.float32)
    return (grad_in, grad_mix, grad_out, grad_gain, grad_head, grad_bias, new_head, new_bias, updated_return_mean, updated_return_scale)
```

```python
import jax
import jax.numpy as jnp
from jax import lax
from jax.sharding import PartitionSpec as P

ACTIONS = 18
TASKS = 57


DISCOUNT = 0.99
BASELINE_COST = 0.5
ENTROPY_COST = 0.01
POPART_PRIOR = 64.0
NORM_EPS = 1e-06


def silu_slope(before):
    sigmoid = jax.nn.sigmoid(before)
    return sigmoid * (1.0 + before * (1.0 - sigmoid))


def discounted_sums(values, factors):

    def advance(running, column):
        latest = column[0] + column[1] * running
        return (latest, latest)

    opening = jnp.zeros((values.shape[0],), jnp.float32)
    ending, stacked = lax.scan(advance, opening, (values.T, factors.T), reverse=True)
    return stacked.T


def task_onehot(task_indices):
    return (task_indices[:, None] == jnp.arange(TASKS, dtype=jnp.int32)[None, :]).astype(
        jnp.float32
    )


def popart_partials(task_indices, rewards, discount_factors):
    returns = discounted_sums(rewards, discount_factors)
    task_table = task_onehot(task_indices)
    counts = jnp.sum(task_table, axis=0) * rewards.shape[1]
    totals = jnp.dot(task_table.T, jnp.sum(returns, axis=1), precision=lax.Precision.HIGHEST)
    squares = jnp.dot(
        task_table.T, jnp.sum(returns * returns, axis=1), precision=lax.Precision.HIGHEST
    )
    return (counts, totals, squares)


def popart_update(counts, totals, squares, pop_mean, pop_scale):
    mixing = counts / (counts + POPART_PRIOR)
    safe_counts = jnp.maximum(counts, 1.0)
    batch_mean = totals / safe_counts
    batch_square = squares / safe_counts
    updated_return_mean = (1.0 - mixing) * pop_mean + mixing * batch_mean
    mean_gap = batch_mean - pop_mean
    variance = (
        (1.0 - mixing) * pop_scale * pop_scale
        + mixing * (batch_square - batch_mean * batch_mean)
        + mixing * (1.0 - mixing) * mean_gap * mean_gap
    )
    return (updated_return_mean, jnp.sqrt(variance))


def rescale_head(w_head, head_bias, pop_mean, pop_scale, updated_return_mean, updated_return_scale):
    scale_ratio = pop_scale / updated_return_scale
    column_scale = jnp.concatenate([jnp.ones((ACTIONS,), jnp.float32), scale_ratio])
    new_head = (w_head.astype(jnp.float32) * column_scale[None, :]).astype(jnp.bfloat16)
    value_bias = (
        pop_scale * head_bias[ACTIONS:] + pop_mean - updated_return_mean
    ) / updated_return_scale
    new_bias = jnp.concatenate([head_bias[:ACTIONS], value_bias])
    return (new_head, new_bias)


def importance_trace_loss(
    head_value_estimates,
    task_indices,
    actions,
    rewards,
    discount_factors,
    behaviour_log_prob,
    updated_return_mean,
    updated_return_scale,
    loss_weighting,
):
    task_table = task_onehot(task_indices)
    env_mean = jnp.dot(task_table, updated_return_mean, precision=lax.Precision.HIGHEST)[:, None]
    env_scale = jnp.dot(task_table, updated_return_scale, precision=lax.Precision.HIGHEST)[:, None]
    logits = head_value_estimates[:, :-1, :ACTIONS]
    norm_values = jnp.sum(head_value_estimates[:, :, ACTIONS:] * task_table[:, None, :], axis=2)
    values = lax.stop_gradient(norm_values * env_scale + env_mean)
    log_total = jnp.log(jnp.sum(jnp.exp(logits), axis=2))
    chosen = actions[:, :, None] == jnp.arange(ACTIONS, dtype=jnp.int32)[None, None, :]
    log_policy = jnp.sum(jnp.where(chosen, logits, 0.0), axis=2) - log_total
    clipped = jnp.minimum(jnp.exp(lax.stop_gradient(log_policy) - behaviour_log_prob), 1.0)
    deltas = clipped * (rewards + discount_factors * values[:, 1:] - values[:, :-1])
    targets = values[:, :-1] + discounted_sums(deltas, discount_factors * clipped)
    following = jnp.concatenate([targets[:, 1:], values[:, -1:]], axis=1)
    advantage = lax.stop_gradient(
        clipped
        * ((rewards + discount_factors * following - env_mean) / env_scale - norm_values[:, :-1])
    )
    normed_targets = lax.stop_gradient((targets - env_mean) / env_scale)
    policy = jnp.exp(logits - log_total[:, :, None])
    entropy = -jnp.sum(policy * (logits - log_total[:, :, None]), axis=2)
    per_frame = (
        -advantage * log_policy
        + 0.5 * BASELINE_COST * (normed_targets - norm_values[:, :-1]) ** 2
        - ENTROPY_COST * entropy
    )
    return loss_weighting * jnp.sum(per_frame)


def powers(axis):
    size = lax.axis_size(axis)
    return [1 << k for k in range(size.bit_length() - 1)]


def swap(block, axis, mask):
    size = lax.axis_size(axis)
    return lax.ppermute(block, axis, [(i, i ^ mask) for i in range(size)])


def side(axis, mask):
    return (lax.axis_index(axis) // mask) % 2


def pair_sum(block, axis, wire):
    for mask in powers(axis):
        sent = block.astype(wire)
        block = sent.astype(jnp.float32) + swap(sent, axis, mask).astype(jnp.float32)
    return block


def collect(block, axis, order):
    shape = block.shape
    for mask in order:
        other = swap(block, axis, mask)
        upper = side(axis, mask) == 1
        block = jnp.stack([jnp.where(upper, other, block), jnp.where(upper, block, other)])
    if not order:
        return block[None]
    leading = list(reversed(order))
    places = [leading.index(mask) for mask in sorted(order, reverse=True)]
    rest = [len(order) + k for k in range(len(shape))]
    return block.transpose(places + rest).reshape((1 << len(order),) + shape)


def scatter_sum(block, axis, order):
    block = block.reshape((2,) * len(order) + block.shape[1:])
    left = sorted(order, reverse=True)
    for mask in order:
        place = left.index(mask)
        mine = side(axis, mask)
        kept = lax.dynamic_index_in_dim(block, mine, place, keepdims=False)
        sent = lax.dynamic_index_in_dim(block, 1 - mine, place, keepdims=False)
        got = swap(sent, axis, mask)
        block = (kept.astype(jnp.float32) + got.astype(jnp.float32)).astype(block.dtype)
        left.remove(mask)
    return block


def orders_of(axis):
    masks = powers(axis)
    return [masks[k:] + masks[:k] for k in range(min(2, len(masks)))] or [[]]


def all_sum(matrix, axis):
    orders = orders_of(axis)
    members = lax.axis_size(axis)
    slabs = jnp.split(matrix, len(orders), axis=0)
    done = []
    for slab, order in zip(slabs, orders):
        parts = slab.reshape((members, slab.shape[0] // members, slab.shape[1]))
        own = scatter_sum(parts, axis, order)
        done.append(collect(own, axis, order[::-1]).reshape(slab.shape))
    return jnp.concatenate(done, axis=0).astype(jnp.float32)


def gather_rows(block, axis):
    orders = orders_of(axis)
    pieces = jnp.split(block, len(orders), axis=0)
    return jnp.concatenate(
        [collect(piece, axis, order) for piece, order in zip(pieces, orders)], axis=1
    )


def gather_shared(block, axis, pair_axis):
    half = block.shape[1] // 2
    second = side(pair_axis, 1)
    own = gather_rows(lax.dynamic_slice_in_dim(block, second * half, half, 1), axis)
    other = swap(own, pair_axis, 1)
    upper = second == 1
    return jnp.concatenate(
        [jnp.where(upper, other, own), jnp.where(upper, own, other)], axis=2
    )


def on_device(
    observations,
    gain,
    w_in,
    w_mix,
    w_out,
    w_head,
    head_bias,
    pop_mean,
    pop_scale,
    task_indices,
    actions,
    rewards,
    episode_ends,
    behaviour_log_prob,
):
    env_count, frames, part_width = observations.shape
    groups = lax.axis_size("tp")
    full_width = part_width * groups
    row_count = env_count * frames
    local_rows = row_count // groups
    own_tokens = observations.reshape(row_count, part_width)
    discount_factors = DISCOUNT * (1.0 - episode_ends.astype(jnp.float32))
    counts, totals, squares = popart_partials(task_indices, rewards, discount_factors)
    counts, totals, squares = pair_sum(
        jnp.stack([counts, totals, squares]), "task", jnp.float32
    )
    updated_return_mean, updated_return_scale = popart_update(
        counts, totals, squares, pop_mean, pop_scale
    )
    new_head, new_bias = rescale_head(
        w_head, head_bias, pop_mean, pop_scale, updated_return_mean, updated_return_scale
    )
    loss_weighting = float(env_count * lax.axis_size("task")) ** (-0.5)
    tokens = lax.all_gather(own_tokens, "tp", axis=1, tiled=True)
    gain_all = collect(gain, "tp", powers("tp")).reshape(full_width)
    tokens, gain_all, new_head, new_bias, updated_return_mean, updated_return_scale = (
        lax.optimization_barrier(
            (tokens, gain_all, new_head, new_bias, updated_return_mean, updated_return_scale)
        )
    )
    tokens_all = gather_shared(tokens, "task", "tp").reshape(-1, full_width)
    row_offset = lax.axis_index("tp") * local_rows
    token_rows = lax.dynamic_slice_in_dim(tokens, row_offset, local_rows, 0)
    pre_in = jnp.dot(tokens, w_in, preferred_element_type=jnp.float32)
    hidden_in = jax.nn.silu(pre_in).astype(jnp.bfloat16)
    hidden_rows = hidden_in
    mix_sum = lax.psum_scatter(
        jnp.dot(hidden_rows, w_mix, preferred_element_type=jnp.float32).astype(jnp.bfloat16),
        "tp",
        scatter_dimension=0,
        tiled=True,
    ).astype(jnp.float32)
    residual = token_rows.astype(jnp.float32) + mix_sum
    inverse = lax.rsqrt(jnp.mean(residual * residual, axis=1, keepdims=True) + NORM_EPS)
    normed = (residual * inverse * gain_all[None, :]).astype(jnp.bfloat16)
    normed_all = lax.all_gather(normed, "tp", axis=0, tiled=True)
    pre_out = jnp.dot(normed_all, w_out, preferred_element_type=jnp.float32)
    hidden_out = jax.nn.silu(pre_out).astype(jnp.bfloat16)
    head_terms = jnp.dot(hidden_out, new_head, preferred_element_type=jnp.float32)
    head_value_estimates = (
        pair_sum(head_terms, "tp", jnp.bfloat16) + new_bias[None, :]
    )
    head_value_estimates = head_value_estimates.reshape(env_count, frames, -1)

    def group_loss(network_outputs):
        return importance_trace_loss(
            network_outputs,
            task_indices,
            actions,
            rewards,
            discount_factors,
            behaviour_log_prob,
            updated_return_mean,
            updated_return_scale,
            loss_weighting,
        )

    loss_value, pullback = jax.vjp(group_loss, head_value_estimates)
    (d_heads,) = pullback(jnp.ones((), jnp.float32))
    d_rounded = d_heads.reshape(row_count, -1).astype(jnp.bfloat16)
    grad_head = jnp.dot(hidden_out.T, d_rounded, preferred_element_type=jnp.float32)
    grad_bias = jnp.sum(d_rounded.astype(jnp.float32), axis=0)
    d_hidden_out = jnp.dot(d_rounded, new_head.T, preferred_element_type=jnp.float32)
    d_pre_out = (d_hidden_out * silu_slope(pre_out)).astype(jnp.bfloat16)
    grad_out = jnp.dot(normed_all.T, d_pre_out, preferred_element_type=jnp.float32)
    d_normed = lax.psum_scatter(
        jnp.dot(d_pre_out, w_out.T, preferred_element_type=jnp.float32).astype(jnp.bfloat16),
        "tp",
        scatter_dimension=0,
        tiled=True,
    ).astype(jnp.float32)
    scaled = d_normed * gain_all[None, :]
    inner_sum = jnp.sum(scaled * residual, axis=1, keepdims=True)
    d_residual = (inverse * scaled - residual * inverse**3 * inner_sum / full_width).astype(
        jnp.bfloat16
    )
    gain_terms = jnp.sum(d_normed * residual * inverse, axis=0)
    arrived = lax.all_gather(d_residual, "tp", axis=0, tiled=True)
    grad_gain = pair_sum(
        scatter_sum(gain_terms.reshape(groups, part_width), "tp", powers("tp")[::-1]),
        "task",
        jnp.float32,
    )
    d_hidden = jnp.dot(arrived, w_mix.T, preferred_element_type=jnp.float32)
    d_pre_in = (d_hidden * silu_slope(pre_in)).astype(jnp.bfloat16)
    d_pre_in, arrived = lax.optimization_barrier((d_pre_in, arrived))
    d_pre_all = gather_rows(d_pre_in, "task").reshape(-1, part_width)
    grad_mix = jnp.dot(hidden_in.T, arrived, preferred_element_type=jnp.float32)
    grad_in = jnp.dot(tokens_all.T, d_pre_all, preferred_element_type=jnp.float32)
    grad_mix = all_sum(grad_mix.astype(jnp.bfloat16), "task")
    grad_out = all_sum(grad_out.astype(jnp.bfloat16), "task")
    grad_head = pair_sum(grad_head, "task", jnp.bfloat16)
    grad_bias = pair_sum(grad_bias, "task", jnp.float32)
    return (
        grad_in,
        grad_mix,
        grad_out,
        grad_gain,
        grad_head,
        grad_bias,
        new_head,
        new_bias,
        updated_return_mean,
        updated_return_scale,
    )


def solution(mesh):
    in_specs = (
        P("task", None, "tp"),
        P("tp"),
        P(None, "tp"),
        P("tp", None),
        P(None, "tp"),
        P("tp", None),
        P(),
        P(),
        P(),
        P("task"),
        P("task", None),
        P("task", None),
        P("task", None),
        P("task", None),
    )
    out_specs = (
        P(None, "tp"),
        P("tp", None),
        P(None, "tp"),
        P("tp"),
        P("tp", None),
        P(),
        P("tp", None),
        P(),
        P(),
        P(),
    )
    return jax.shard_map(
        on_device, mesh=mesh, in_specs=in_specs, out_specs=out_specs, check_vma=False
    )
```

```python
import jax
import jax.numpy as jnp
from jax import lax
from jax.sharding import PartitionSpec as P

ACTIONS = 18
TASKS = 57


DISCOUNT = 0.99
BASELINE_COST = 0.5
ENTROPY_COST = 0.01
POPART_PRIOR = 64.0
NORM_EPS = 1e-06


def silu_slope(before):
    sigmoid = jax.nn.sigmoid(before)
    return sigmoid * (1.0 + before * (1.0 - sigmoid))


def discounted_sums(values, factors):
    length = values.shape[1]
    step = 1
    while step < length:
        later = lambda rows: jnp.pad(rows[:, step:], ((0, 0), (0, step)))
        values = values + factors * later(values)
        factors = factors * later(factors)
        step *= 2
    return values


def task_onehot(task_indices):
    return (task_indices[:, None] == jnp.arange(TASKS, dtype=jnp.int32)[None, :]).astype(
        jnp.float32
    )


def popart_partials(task_indices, rewards, discount_factors):
    returns = discounted_sums(rewards, discount_factors)
    task_table = task_onehot(task_indices)
    counts = jnp.sum(task_table, axis=0) * rewards.shape[1]
    totals = jnp.dot(task_table.T, jnp.sum(returns, axis=1), precision=lax.Precision.HIGHEST)
    squares = jnp.dot(
        task_table.T, jnp.sum(returns * returns, axis=1), precision=lax.Precision.HIGHEST
    )
    return (counts, totals, squares)


def popart_update(counts, totals, squares, pop_mean, pop_scale):
    mixing = counts / (counts + POPART_PRIOR)
    safe_counts = jnp.maximum(counts, 1.0)
    batch_mean = totals / safe_counts
    batch_square = squares / safe_counts
    updated_return_mean = (1.0 - mixing) * pop_mean + mixing * batch_mean
    mean_gap = batch_mean - pop_mean
    variance = (
        (1.0 - mixing) * pop_scale * pop_scale
        + mixing * (batch_square - batch_mean * batch_mean)
        + mixing * (1.0 - mixing) * mean_gap * mean_gap
    )
    return (updated_return_mean, jnp.sqrt(variance))


def rescale_head(w_head, head_bias, pop_mean, pop_scale, updated_return_mean, updated_return_scale):
    scale_ratio = pop_scale / updated_return_scale
    column_scale = jnp.concatenate([jnp.ones((ACTIONS,), jnp.float32), scale_ratio])
    new_head = (w_head.astype(jnp.float32) * column_scale[None, :]).astype(jnp.bfloat16)
    value_bias = (
        pop_scale * head_bias[ACTIONS:] + pop_mean - updated_return_mean
    ) / updated_return_scale
    new_bias = jnp.concatenate([head_bias[:ACTIONS], value_bias])
    return (new_head, new_bias)


def importance_trace_loss(
    head_value_estimates,
    task_indices,
    actions,
    rewards,
    discount_factors,
    behaviour_log_prob,
    updated_return_mean,
    updated_return_scale,
    loss_weighting,
):
    task_table = task_onehot(task_indices)
    env_mean = jnp.dot(task_table, updated_return_mean, precision=lax.Precision.HIGHEST)[:, None]
    env_scale = jnp.dot(task_table, updated_return_scale, precision=lax.Precision.HIGHEST)[:, None]
    logits = head_value_estimates[:, :-1, :ACTIONS]
    norm_values = jnp.sum(head_value_estimates[:, :, ACTIONS:] * task_table[:, None, :], axis=2)
    values = lax.stop_gradient(norm_values * env_scale + env_mean)
    log_total = jnp.log(jnp.sum(jnp.exp(logits), axis=2))
    chosen = actions[:, :, None] == jnp.arange(ACTIONS, dtype=jnp.int32)[None, None, :]
    log_policy = jnp.sum(jnp.where(chosen, logits, 0.0), axis=2) - log_total
    clipped = jnp.minimum(jnp.exp(lax.stop_gradient(log_policy) - behaviour_log_prob), 1.0)
    deltas = clipped * (rewards + discount_factors * values[:, 1:] - values[:, :-1])
    targets = values[:, :-1] + discounted_sums(deltas, discount_factors * clipped)
    following = jnp.concatenate([targets[:, 1:], values[:, -1:]], axis=1)
    advantage = lax.stop_gradient(
        clipped
        * ((rewards + discount_factors * following - env_mean) / env_scale - norm_values[:, :-1])
    )
    normed_targets = lax.stop_gradient((targets - env_mean) / env_scale)
    policy = jnp.exp(logits - log_total[:, :, None])
    entropy = -jnp.sum(policy * (logits - log_total[:, :, None]), axis=2)
    per_frame = (
        -advantage * log_policy
        + 0.5 * BASELINE_COST * (normed_targets - norm_values[:, :-1]) ** 2
        - ENTROPY_COST * entropy
    )
    return loss_weighting * jnp.sum(per_frame)


def powers(axis):
    size = lax.axis_size(axis)
    return [1 << k for k in range(size.bit_length() - 1)]


def swap(block, axis, mask):
    size = lax.axis_size(axis)
    return lax.ppermute(block, axis, [(i, i ^ mask) for i in range(size)])


def side(axis, mask):
    return (lax.axis_index(axis) // mask) % 2


def pair_sum(block, axis, wire):
    for mask in powers(axis):
        sent = block.astype(wire)
        block = sent.astype(jnp.float32) + swap(sent, axis, mask).astype(jnp.float32)
    return block


def collect(block, axis, order):
    shape = block.shape
    for mask in order:
        other = swap(block, axis, mask)
        upper = side(axis, mask) == 1
        block = jnp.stack([jnp.where(upper, other, block), jnp.where(upper, block, other)])
    if not order:
        return block[None]
    leading = list(reversed(order))
    places = [leading.index(mask) for mask in sorted(order, reverse=True)]
    rest = [len(order) + k for k in range(len(shape))]
    return block.transpose(places + rest).reshape((1 << len(order),) + shape)


def scatter_step(block, axis, left, mask):
    place = left.index(mask)
    mine = side(axis, mask)
    kept = lax.dynamic_index_in_dim(block, mine, place, keepdims=False)
    sent = lax.dynamic_index_in_dim(block, 1 - mine, place, keepdims=False)
    got = swap(sent, axis, mask)
    left.remove(mask)
    return (kept.astype(jnp.float32) + got.astype(jnp.float32)).astype(block.dtype)


def scatter_sum(block, axis, order):
    block = block.reshape((2,) * len(order) + block.shape[1:])
    left = sorted(order, reverse=True)
    for mask in order:
        block = scatter_step(block, axis, left, mask)
    return block


def orders_of(axis):
    masks = powers(axis)
    return [masks[k:] + masks[:k] for k in range(min(2, len(masks)))]


def sum_first(matrix, axis):
    orders = orders_of(axis)
    slabs = []
    for slab, order in zip(jnp.split(matrix, len(orders), axis=0), orders):
        members = 1 << len(order)
        parts = slab.reshape((2,) * len(order) + (slab.shape[0] // members, slab.shape[1]))
        left = sorted(order, reverse=True)
        slabs.append(scatter_step(parts, axis, left, order[0]))
    return slabs


def sum_middle(slabs, axis):
    parts = []
    for slab, order in zip(slabs, orders_of(axis)):
        left = sorted(order[1:], reverse=True)
        for mask in order[1:]:
            slab = scatter_step(slab, axis, left, mask)
        parts.append(slab)
    return parts


def sum_last(parts, axis):
    done = []
    for part, order in zip(parts, orders_of(axis)):
        done.append(collect(part, axis, order[::-1]).reshape(-1, part.shape[1]))
    return jnp.concatenate(done, axis=0).astype(jnp.float32)


def place_rows(own, others, axis):
    index = lax.axis_index(axis)
    table = jnp.zeros((lax.axis_size(axis),) + own.shape, own.dtype)
    for mask, block in {0: own, **others}.items():
        table = lax.dynamic_update_index_in_dim(table, block, index ^ mask, 0)
    return table


def on_device(
    observations,
    gain,
    w_in,
    w_mix,
    w_out,
    w_head,
    head_bias,
    pop_mean,
    pop_scale,
    task_indices,
    actions,
    rewards,
    episode_ends,
    behaviour_log_prob,
):
    env_count, frames, part_width = observations.shape
    groups = lax.axis_size("tp")
    full_width = part_width * groups
    row_count = env_count * frames
    local_rows = row_count // groups
    own_tokens = observations.reshape(row_count, part_width)
    discount_factors = DISCOUNT * (1.0 - episode_ends.astype(jnp.float32))
    counts, totals, squares = popart_partials(task_indices, rewards, discount_factors)
    counts, totals, squares = pair_sum(
        jnp.stack([counts, totals, squares]), "task", jnp.float32
    )
    updated_return_mean, updated_return_scale = popart_update(
        counts, totals, squares, pop_mean, pop_scale
    )
    new_head, new_bias = rescale_head(
        w_head, head_bias, pop_mean, pop_scale, updated_return_mean, updated_return_scale
    )
    loss_weighting = float(env_count * lax.axis_size("task")) ** (-0.5)
    tokens = lax.all_gather(own_tokens, "tp", axis=1, tiled=True)
    gain_all = collect(gain, "tp", powers("tp")).reshape(full_width)
    tokens, gain_all, new_head, new_bias, updated_return_mean, updated_return_scale = (
        lax.optimization_barrier(
            (tokens, gain_all, new_head, new_bias, updated_return_mean, updated_return_scale)
        )
    )
    half = full_width // 2
    second = side("tp", 1)
    turned = lax.optimization_barrier(tokens.T)
    own_half = lax.dynamic_slice_in_dim(turned, second * half, half, 0)
    masks = range(1, lax.axis_size("task"))
    near = {mask: swap(own_half, "task", mask) for mask in powers("task")}
    far = {mask: swap(own_half, "task", mask) for mask in masks if mask not in near}
    row_offset = lax.axis_index("tp") * local_rows
    token_rows = lax.dynamic_slice_in_dim(tokens, row_offset, local_rows, 0)
    pre_in = jnp.dot(tokens, w_in, preferred_element_type=jnp.float32)
    hidden_in = jax.nn.silu(pre_in).astype(jnp.bfloat16)
    hidden_rows = hidden_in
    mix_sum = lax.psum_scatter(
        jnp.dot(hidden_rows, w_mix, preferred_element_type=jnp.float32).astype(jnp.bfloat16),
        "tp",
        scatter_dimension=0,
        tiled=True,
    ).astype(jnp.float32)
    residual = token_rows.astype(jnp.float32) + mix_sum
    inverse = lax.rsqrt(jnp.mean(residual * residual, axis=1, keepdims=True) + NORM_EPS)
    normed = (residual * inverse * gain_all[None, :]).astype(jnp.bfloat16)
    normed, near = lax.optimization_barrier((normed, near))
    near_pair = {mask: swap(block, "tp", 1) for mask, block in near.items()}
    normed_all = lax.all_gather(normed, "tp", axis=0, tiled=True)
    place = lax.axis_index("task")
    table = jnp.zeros((2, half, lax.axis_size("task") * row_count), tokens.dtype)
    table = lax.dynamic_update_slice(
        table, turned.reshape(2, half, row_count), (0, 0, place * row_count)
    )
    for mask, block in near.items():
        table = lax.dynamic_update_slice(
            table, block[None], (second, 0, (place ^ mask) * row_count)
        )
    normed_all, far, near_pair, table = lax.optimization_barrier(
        (normed_all, far, near_pair, table)
    )
    far_pair = {mask: swap(block, "tp", 1) for mask, block in far.items()}
    pre_out = jnp.dot(normed_all, w_out, preferred_element_type=jnp.float32)
    hidden_out = jax.nn.silu(pre_out).astype(jnp.bfloat16)
    head_terms = jnp.dot(hidden_out, new_head, preferred_element_type=jnp.float32)
    head_value_estimates = (
        pair_sum(head_terms, "tp", jnp.bfloat16) + new_bias[None, :]
    )
    head_value_estimates = head_value_estimates.reshape(env_count, frames, -1)

    def group_loss(network_outputs):
        return importance_trace_loss(
            network_outputs,
            task_indices,
            actions,
            rewards,
            discount_factors,
            behaviour_log_prob,
            updated_return_mean,
            updated_return_scale,
            loss_weighting,
        )

    loss_value, pullback = jax.vjp(group_loss, head_value_estimates)
    (d_heads,) = pullback(jnp.ones((), jnp.float32))
    d_rounded = d_heads.reshape(row_count, -1).astype(jnp.bfloat16)
    grad_head = jnp.dot(hidden_out.T, d_rounded, preferred_element_type=jnp.float32)
    grad_bias = jnp.sum(d_rounded.astype(jnp.float32), axis=0)
    d_hidden_out = jnp.dot(d_rounded, new_head.T, preferred_element_type=jnp.float32)
    d_pre_out = (d_hidden_out * silu_slope(pre_out)).astype(jnp.bfloat16)
    d_pre_out, far_pair = lax.optimization_barrier((d_pre_out, far_pair))
    grad_out = jnp.dot(normed_all.T, d_pre_out, preferred_element_type=jnp.float32)
    grad_out, table, far, near_pair, far_pair = lax.optimization_barrier(
        (grad_out.astype(jnp.bfloat16), table, far, near_pair, far_pair)
    )
    slabs = sum_first(grad_out, "task")
    for blocks, at in ((far, second), (near_pair, 1 - second), (far_pair, 1 - second)):
        for mask, block in blocks.items():
            table = lax.dynamic_update_slice(
                table, block[None], (at, 0, (place ^ mask) * row_count)
            )
    d_normed = lax.psum_scatter(
        jnp.dot(d_pre_out, w_out.T, preferred_element_type=jnp.float32).astype(jnp.bfloat16),
        "tp",
        scatter_dimension=0,
        tiled=True,
    ).astype(jnp.float32)
    scaled = d_normed * gain_all[None, :]
    inner_sum = jnp.sum(scaled * residual, axis=1, keepdims=True)
    d_residual = (inverse * scaled - residual * inverse**3 * inner_sum / full_width).astype(
        jnp.bfloat16
    )
    gain_terms = jnp.sum(d_normed * residual * inverse, axis=0)
    d_residual, slabs, table = lax.optimization_barrier((d_residual, slabs, table))
    arrived = lax.all_gather(d_residual, "tp", axis=0, tiled=True)
    out_parts = sum_middle(slabs, "task")
    grad_head = pair_sum(grad_head, "task", jnp.bfloat16)
    grad_bias = pair_sum(grad_bias, "task", jnp.float32)
    grad_gain = pair_sum(
        scatter_sum(gain_terms.reshape(groups, part_width), "tp", powers("tp")[::-1]),
        "task",
        jnp.float32,
    )
    arrived, out_parts, grad_head, grad_bias, grad_gain = lax.optimization_barrier(
        (arrived, out_parts, grad_head, grad_bias, grad_gain)
    )
    d_hidden = jnp.dot(arrived, w_mix.T, preferred_element_type=jnp.float32)
    d_pre_in = (d_hidden * silu_slope(pre_in)).astype(jnp.bfloat16)
    d_pre_in, arrived = lax.optimization_barrier((d_pre_in, arrived))
    d_pre_others = {mask: swap(d_pre_in, "task", mask) for mask in masks}
    d_pre_all = place_rows(d_pre_in, d_pre_others, "task").reshape(-1, part_width)
    grad_mix = jnp.dot(hidden_in.T, arrived, preferred_element_type=jnp.float32)
    slabs = sum_first(grad_mix.astype(jnp.bfloat16), "task")
    grad_in = jnp.dot(
        table.reshape(full_width, -1), d_pre_all, preferred_element_type=jnp.float32
    )
    grad_out = sum_last(out_parts, "task")
    grad_mix = sum_last(sum_middle(slabs, "task"), "task")
    return (
        grad_in,
        grad_mix,
        grad_out,
        grad_gain,
        grad_head,
        grad_bias,
        new_head,
        new_bias,
        updated_return_mean,
        updated_return_scale,
    )


def solution(mesh):
    in_specs = (
        P("task", None, "tp"),
        P("tp"),
        P(None, "tp"),
        P("tp", None),
        P(None, "tp"),
        P("tp", None),
        P(),
        P(),
        P(),
        P("task"),
        P("task", None),
        P("task", None),
        P("task", None),
        P("task", None),
    )
    out_specs = (
        P(None, "tp"),
        P("tp", None),
        P(None, "tp"),
        P("tp"),
        P("tp", None),
        P(),
        P("tp", None),
        P(),
        P(),
        P(),
    )
    return jax.shard_map(
        on_device, mesh=mesh, in_specs=in_specs, out_specs=out_specs, check_vma=False
    )
```
